32 devices in a mesh: groups: 2 (over y), wide: 8 (over z, x), narrow: 2 (over core).
Axes of the slice: x: 2, y: 2, z: 4, core: 2. Of those that a mesh axis runs over, the one named last changes fastest.
Arguments:
- hidden_in: bfloat16 [6400, 1024], P(('groups', 'wide')), parts along dimension 0, may hold values from -6 to 6
- ffn_gain: bfloat16 [1024], replicated, may hold values from 0.5 to 1.5
- wi_gate: bfloat16 [1024, 2816], P('wide', 'narrow'), may hold values from -0.1875 to 0.1875
- wi_up: bfloat16 [1024, 2816], P('wide', 'narrow'), may hold values from -0.1875 to 0.1875
- wo_down: bfloat16 [2816, 1024], P('narrow', 'wide'), may hold values from -0.109375 to 0.109375
- final_gain: bfloat16 [1024], replicated, may hold values from 0.5 to 1.5
- key_w: bfloat16 [1024, 1024], P('wide', 'narrow'), may hold values from -0.1875 to 0.1875
- value_w: bfloat16 [1024, 1024], P('wide', 'narrow'), may hold values from -0.1875 to 0.1875
- query_w: bfloat16 [1024, 1024], P('wide', 'narrow'), may hold values from -8 to 8
- out_w: bfloat16 [1024, 1024], P('narrow', 'wide'), may hold values from -0.1875 to 0.1875
- dec_gain: bfloat16 [1024], replicated, may hold values from 0.5 to 1.5
- embed: bfloat16 [32128, 1024], P('wide'), may hold values from -6 to 6
- lengths: int32 [32], P(('groups', 'wide')), parts along dimension 0, may hold values from 40 to 200
- answer_ids: int32 [8, 32], P('groups'), parts along dimension 0, may hold values from 0 to 32127
Outputs:
- memory: bfloat16 [6400, 1024], P(('groups', 'wide')), parts along dimension 0
- decoded: bfloat16 [256, 1024], P('groups', 'narrow'), parts along dimension 0
The draws below stay inside these ranges and needn't reach their ends.
There are 2 independent parts, one for each index of `groups`. The reference program is written for one: setup_inputs(seed, part) draws one part's arguments, and reference() takes and returns one part's arrays. A program takes and returns all parts, laid end to end along the dimension named above; an argument that names none is the same for every part. Nothing has to cross between parts.
All inputs are finite; a program needn't handle non-finite values.
Results may differ from the reference program's by a relative error of at most 0.0095.
The reference program's roundings to bfloat16 on the way (of `enc_in`, `inner`, `embedded`, `dec_in`, `query` and `attended`) count: a program that leaves them out, or rounds other values in their place, can miss the bound.
Values may be sent and summed in bfloat16 or wider, within the bound.
No kernel may reach another device: no remote copies, remote signals or barrier semaphores. Data moves between devices by JAX's collectives and lax.ppermute only.
A program may use at most 64 MiB of HBM per device.

```python
import math
import jax
import jax.numpy as jnp
from jax import lax

D = 1024
HEADS = 16
HEAD_DIM = 64
FF = 2816
VOCAB = 32128
SEG = 200
QUEST = 4
ANS = 32
PASSAGES = 16
TOKENS = 3200
PER_Q = 4
QROWS = 128


def draw_query_w(key, part):
    base = jax.random.normal(jax.random.fold_in(key, 11), (D, D), jnp.float32)
    picked = jax.random.permutation(jax.random.fold_in(key, 12), HEADS)[:2]
    column_head = jnp.arange(D, dtype=jnp.int32) // HEAD_DIM
    strengths = jnp.array([60.0, 100.0], jnp.float32)
    factor = jnp.ones((D,), jnp.float32)
    factor = jnp.where(column_head == picked[0], strengths[0], factor)
    factor = jnp.where(column_head == picked[1], strengths[1], factor)
    scaled = base * (factor / math.sqrt(D))[None, :]
    return jnp.clip(scaled, -8.0, 8.0).astype(jnp.bfloat16)


def set_ends(result, own_key, least, largest):
    place = [jax.random.randint(jax.random.fold_in(own_key, axis), (), 0, length) for axis, length in enumerate(result.shape)]
    longest = result.shape.index(max(result.shape))
    neighbour = place[:longest] + [(place[longest] + 1) % result.shape[longest]] + place[longest + 1:]
    return result.at[tuple(place)].set(least).at[tuple(neighbour)].set(largest)


def shard_levels(rng, shape, split, low, top_value):
    factor_of, own = 1.0, jax.random.fold_in(rng, 6)
    for axis_at, shards_of in split:
        heights = jnp.exp(jax.random.uniform(jax.random.fold_in(own, axis_at), (shards_of,), jnp.float32, low / len(split), top_value / len(split)))
        factor_of = factor_of * jnp.repeat(heights, shape[axis_at] // shards_of).reshape([-1 if axis == axis_at else 1 for axis in range(len(shape))])
    return factor_of


def normal_values(own_key, dims, width, reach, shards=(), kind=jnp.bfloat16):
    drawn = width * jax.random.normal(own_key, dims, jnp.float32)
    if shards:
        drawn = drawn * shard_levels(own_key, dims, shards, -0.22, 0.18)
    return jnp.clip(drawn, -reach, reach).astype(kind)


def setup_inputs(seed: int = 0, part: int = 0) -> dict:
    splits = jax.random.split(jax.random.key(seed), 15)
    part_keys = jax.random.split(jax.random.fold_in(splits[14], part), 15)
    return {
        "hidden_in": normal_values(part_keys[0], (TOKENS, D), 1.0, 6.0, ((0, 8),)),
        "ffn_gain": jnp.clip(1.0 + 0.1 * jax.random.normal(splits[1], (D,), jnp.float32), 0.5, 1.5).astype(jnp.bfloat16),
        "wi_gate": normal_values(splits[2], (D, FF), D ** -0.5, 0.1875, ((0, 8), (1, 2))),
        "wi_up": normal_values(splits[3], (D, FF), D ** -0.5, 0.1875, ((0, 8), (1, 2))),
        "wo_down": normal_values(splits[4], (FF, D), FF ** -0.5, 0.109375, ((0, 2), (1, 8))),
        "final_gain": jnp.clip(1.0 + 0.1 * jax.random.normal(splits[5], (D,), jnp.float32), 0.5, 1.5).astype(jnp.bfloat16),
        "key_w": normal_values(splits[6], (D, D), D ** -0.5, 0.1875, ((0, 8), (1, 2))),
        "value_w": normal_values(splits[7], (D, D), D ** -0.5, 0.1875, ((0, 8), (1, 2))),
        "query_w": draw_query_w(jax.random.fold_in(splits[14], 71), part),
        "out_w": normal_values(splits[9], (D, D), D ** -0.5, 0.1875, ((0, 2), (1, 8))),
        "dec_gain": jnp.clip(1.0 + 0.1 * jax.random.normal(splits[10], (D,), jnp.float32), 0.5, 1.5).astype(jnp.bfloat16),
        "embed": normal_values(splits[11], (VOCAB, D), 1.0, 6.0, ((0, 8),)),
        "lengths": set_ends(jax.random.randint(part_keys[12], (PASSAGES,), SEG // 5, SEG + 1), jax.random.fold_in(part_keys[12], 1), SEG // 5, SEG).astype(jnp.int32),
        "answer_ids": set_ends(jax.random.randint(part_keys[13], (QUEST, ANS), 0, VOCAB), jax.random.fold_in(part_keys[13], 1), 0, VOCAB - 1).astype(jnp.int32),
    }


EPS = 1e-06
FLOOR = -1e+30

def rms_scale(values, gain):
    mean_square = lax.optimization_barrier(jnp.mean(values * values, axis=-1, keepdims=True))
    return values * lax.rsqrt(mean_square + EPS) * gain.astype(jnp.float32)

def reference(hidden_in, ffn_gain, wi_gate, wi_up, wo_down, final_gain, key_w, value_w, query_w, out_w, dec_gain, embed, lengths, answer_ids):

    def encode(block):
        resid_in = block.astype(jnp.float32)
        enc_in = rms_scale(resid_in, ffn_gain).astype(jnp.bfloat16)
        gate = jnp.dot(enc_in, wi_gate, preferred_element_type=jnp.float32)
        up = jnp.dot(enc_in, wi_up, preferred_element_type=jnp.float32)
        inner = (jax.nn.gelu(gate, approximate=True) * up).astype(jnp.bfloat16)
        resid = resid_in + jnp.dot(inner, wo_down, preferred_element_type=jnp.float32)
        memory = rms_scale(resid, final_gain).astype(jnp.bfloat16)
        keys = jnp.dot(memory, key_w, preferred_element_type=jnp.float32).astype(jnp.bfloat16)
        values = jnp.dot(memory, value_w, preferred_element_type=jnp.float32).astype(jnp.bfloat16)
        return (memory, keys, values)
    blocks = hidden_in.reshape(PASSAGES, SEG, D)
    memory, keys, values = lax.map(encode, blocks)
    flat_ids = answer_ids.reshape(QROWS)
    embedded = jnp.take(embed, flat_ids, axis=0)
    dec_in = rms_scale(embedded.astype(jnp.float32), dec_gain).astype(jnp.bfloat16)
    query = jnp.dot(dec_in, query_w, preferred_element_type=jnp.float32).astype(jnp.bfloat16)
    query_four = query.reshape(QUEST, ANS, HEADS, HEAD_DIM).astype(jnp.float32)
    keys_four = keys.reshape(QUEST, PER_Q * SEG, HEADS, HEAD_DIM).astype(jnp.float32)
    values_four = values.reshape(QUEST, PER_Q * SEG, HEADS, HEAD_DIM).astype(jnp.float32)
    position = jnp.arange(SEG, dtype=jnp.int32)
    live = (position[None, :] < lengths[:, None]).reshape(QUEST, PER_Q * SEG)
    scores = jnp.einsum('qahd,qkhd->qahk', query_four, keys_four, precision=lax.Precision.HIGHEST) * (1.0 / math.sqrt(HEAD_DIM))
    scores = jnp.where(live[:, None, None, :], scores, FLOOR)
    weights = jax.nn.softmax(scores, axis=-1)
    attended = jnp.einsum('qahk,qkhd->qahd', weights, values_four, precision=lax.Precision.HIGHEST)
    attended = attended.reshape(QROWS, D).astype(jnp.bfloat16)
    decoded = embedded.astype(jnp.float32) + jnp.dot(attended, out_w, preferred_element_type=jnp.float32)
    return (memory.reshape(TOKENS, D), decoded.astype(jnp.bfloat16))
```

```python
import math

import jax
import jax.numpy as jnp
from jax import lax
from jax.sharding import PartitionSpec as P

HEAD_DIM = 64
QUEST = 4


EPS = 1e-06
FLOOR = -1e30


LANES = 128


def swap(array, axis):
    return lax.ppermute(array, axis, [(0, 1), (1, 0)])


def swap_pair(array):
    size = lax.axis_size("wide")
    return lax.ppermute(array, "wide", [(i, i ^ 1) for i in range(size)])


def line_sources(outer):
    table = []
    for place in range(outer):
        others = [d for d in range(-place, outer - place) if d != 0]
        table.append([0] + sorted(others, key=lambda d: (abs(d), d)))
    return table


def spread(shard):
    size = lax.axis_size("wide")
    outer = size // 2
    table = line_sources(outer)
    place = lax.axis_index("wide") // 2
    above = [(i, i + 2) for i in range(size - 2)]
    below = [(i + 2, i) for i in range(size - 2)]
    held = {0: shard}
    for step in range(1, outer):
        held[-step] = lax.ppermute(held[1 - step], "wide", above)
        held[step] = lax.ppermute(held[step - 1], "wide", below)
    blocks = []
    for slot in range(outer):
        wanted = sorted({table[p][slot] for p in range(outer)})
        chosen = held[wanted[0]]
        mine = jnp.array([table[p][slot] for p in range(outer)], jnp.int32)[place]
        for distance in wanted[1:]:
            chosen = jnp.where(mine == distance, held[distance], chosen)
        blocks += [chosen, swap_pair(chosen)]
    return blocks


def block_order():
    size = lax.axis_size("wide")
    outer = size // 2
    table = line_sources(outer)
    index = lax.axis_index("wide")
    place, side = index // 2, index % 2
    order, where_is = [], []
    for slot in range(outer):
        source = jnp.array([p + table[p][slot] for p in range(outer)], jnp.int32)[place]
        order += [2 * source + side, 2 * source + 1 - side]
    for target in range(outer):
        slots = [table[p].index(target - p) for p in range(outer)]
        slot = jnp.array(slots, jnp.int32)[place]
        where_is += [2 * slot + side, 2 * slot + 1 - side]
    return order, where_is


def take_blocks(array, order):
    width = array.shape[1] // len(order)
    return jnp.concatenate(
        [lax.dynamic_slice_in_dim(array, i * width, width, 1) for i in order], axis=1
    )


def half_of(array, which, axis):
    first, second = jnp.split(array, 2, axis)
    return jnp.where(which == 0, first, second)


def join_rows(first_half, which):
    other = swap(first_half, "narrow")
    return jnp.concatenate(
        [jnp.where(which == 0, first_half, other), jnp.where(which == 0, other, first_half)], 0
    )


def gated(enc, gate_w, up_w):
    gate = add_rows(enc, gate_w)
    up = add_rows(enc, up_w)
    return (jax.nn.gelu(gate, approximate=True) * up).astype(jnp.bfloat16)


def sum_cores(partial, core):
    keep = half_of(partial, core, 0)
    send = half_of(partial, 1 - core, 0)
    return keep + swap(send, "narrow")


def ffn_shared(enc_in, wi_gate, wi_up, wo_down, core):
    twin = lax.axis_index("groups")
    enc_twin = swap(enc_in, "groups")
    into = jnp.concatenate([half_of(wi_gate, twin, 1), half_of(wi_up, twin, 1)], 1)
    into_blocks = spread(into)
    down_blocks = spread(half_of(wo_down, twin, 0))
    order, where_is = block_order()
    width = into.shape[1] // 2
    gate_w = jnp.concatenate([b[:, :width] for b in into_blocks], 0)
    up_w = jnp.concatenate([b[:, width:] for b in into_blocks], 0)
    down_w = jnp.concatenate(down_blocks, 1)
    away = sum_cores(add_rows(gated(take_blocks(enc_twin, order), gate_w, up_w), down_w), core)
    back = swap(away, "groups")
    here = sum_cores(add_rows(gated(take_blocks(enc_in, order), gate_w, up_w), down_w), core)
    return take_blocks(here + back, where_is)


def ffn_whole(enc_in, wi_gate, wi_up, wo_down, core):
    gate_w = lax.all_gather(wi_gate, "wide", axis=0, tiled=True)
    up_w = lax.all_gather(wi_up, "wide", axis=0, tiled=True)
    down_w = lax.all_gather(wo_down, "wide", axis=1, tiled=True)
    return sum_cores(add_rows(gated(enc_in, gate_w, up_w), down_w), core)


def rms_scale(values, gain):
    mean_square = jnp.mean(values * values, axis=-1, keepdims=True)
    return values * lax.rsqrt(mean_square + EPS) * gain.astype(jnp.float32)


def add_rows(left, piece):
    return jnp.dot(left, piece, preferred_element_type=jnp.float32)


def join_partial(first, second):
    top_first, total_first, acc_first = first
    top_second, total_second, acc_second = second
    top = jnp.maximum(top_first, top_second)
    factor_first = jnp.exp(top_first - top)
    factor_second = jnp.exp(top_second - top)
    width = acc_first.shape[1] // top.shape[1]
    total = total_first * factor_first + total_second * factor_second
    acc = acc_first * jnp.repeat(factor_first, width, axis=1) + acc_second * jnp.repeat(
        factor_second, width, axis=1
    )
    return (top, total, acc)


def per_device(
    hidden_in,
    ffn_gain,
    wi_gate,
    wi_up,
    wo_down,
    final_gain,
    key_w,
    value_w,
    query_w,
    out_w,
    dec_gain,
    embed,
    lengths,
    answer_ids,
):
    rows = hidden_in.shape[0]
    features = hidden_in.shape[1]
    resid_in = hidden_in.astype(jnp.float32)
    enc_in = rms_scale(resid_in, ffn_gain).astype(jnp.bfloat16)

    core = lax.axis_index("narrow")
    size = lax.axis_size("wide")
    pass_dev = lengths.shape[0]
    members = size // QUEST
    question = lax.axis_index("wide") // members
    answers = answer_ids.shape[1]
    qrows = answer_ids.shape[0] * answers
    proj_cols = key_w.shape[1]
    heads_local = proj_cols // HEAD_DIM

    projections = lax.all_gather(
        jnp.concatenate([key_w, value_w, query_w], 1), "wide", axis=0, tiled=True
    )
    out_full = lax.all_gather(out_w, "wide", axis=1, tiled=True)

    vocab_rows = embed.shape[0]
    local_ids = answer_ids.reshape(qrows) - lax.axis_index("wide") * vocab_rows
    onehot = (local_ids[:, None] == jnp.arange(vocab_rows, dtype=jnp.int32)[None, :]).astype(
        jnp.bfloat16
    )
    found = add_rows(onehot, embed).astype(jnp.bfloat16)
    sent = jnp.repeat(found.reshape(QUEST, answers, features), members, axis=0)
    embedded = jnp.sum(
        lax.all_to_all(sent, "wide", 0, 0).astype(jnp.float32), axis=0
    )
    dec_in = rms_scale(embedded, dec_gain).astype(jnp.bfloat16)

    shared = (
        lax.axis_size("groups") == 2 and size % 2 == 0 and wi_gate.shape[0] % LANES == 0
    )
    ffn = ffn_shared if shared else ffn_whole
    added = ffn(enc_in, wi_gate, wi_up, wo_down, core)
    resid = half_of(resid_in, core, 0) + added
    memory = join_rows(rms_scale(resid, final_gain).astype(jnp.bfloat16), core)

    query = add_rows(dec_in, projections[:, 2 * proj_cols :]).astype(jnp.bfloat16)
    keys = add_rows(memory, projections[:, :proj_cols]).astype(jnp.bfloat16)
    values = add_rows(memory, projections[:, proj_cols : 2 * proj_cols]).astype(jnp.bfloat16)
    query_three = query.reshape(answers, heads_local, HEAD_DIM)
    keys_three = keys.reshape(rows, heads_local, HEAD_DIM)
    values_three = values.reshape(rows, heads_local, HEAD_DIM).astype(jnp.float32)
    scores = jnp.einsum(
        "ahd,khd->ahk", query_three, keys_three, preferred_element_type=jnp.float32
    ) * (1.0 / math.sqrt(HEAD_DIM))
    passage_len = rows // pass_dev
    live = (jnp.arange(passage_len, dtype=jnp.int32)[None, :] < lengths[:, None]).reshape(rows)
    scores = jnp.where(live[None, None, :], scores, FLOOR)
    top = jnp.max(scores, axis=2)
    weights = jnp.exp(scores - top[:, :, None])
    total = jnp.sum(weights, axis=2)
    acc = jnp.einsum(
        "ahk,khd->ahd", weights, values_three, precision=lax.Precision.HIGHEST
    ).reshape(answers, proj_cols)

    packed = jnp.concatenate([acc, top, total], 1)
    ring = [(i, i // members * members + (i + 1) % members) for i in range(size)]
    state = (top, total, acc)
    for _ in range(1, members):
        packed = lax.ppermute(packed, "wide", ring)
        piece = (
            packed[:, proj_cols : proj_cols + heads_local],
            packed[:, proj_cols + heads_local :],
            packed[:, :proj_cols],
        )
        state = join_partial(state, piece)
    _, total, acc = state
    attended = (acc / jnp.repeat(total, HEAD_DIM, axis=1)).astype(jnp.bfloat16)
    partial_out = add_rows(attended, out_full)
    share_out = half_of(partial_out, core, 1) + swap(half_of(partial_out, 1 - core, 1), "narrow")
    mine = (half_of(embedded, core, 1) + share_out).astype(jnp.bfloat16)
    decoded = jnp.zeros((qrows, mine.shape[1]), jnp.bfloat16)
    decoded = lax.dynamic_update_slice_in_dim(decoded, mine, question * answers, 0)
    for step in range(1, QUEST):
        shift = [(i, (i + step * members) % size) for i in range(size)]
        other = lax.ppermute(mine, "wide", shift)
        source = (question - step) % QUEST
        decoded = lax.dynamic_update_slice_in_dim(decoded, other, source * answers, 0)
    return (memory, decoded)


def solution(mesh):
    placed = (
        P(("groups", "wide"), None),
        P(),
        P("wide", "narrow"),
        P("wide", "narrow"),
        P("narrow", "wide"),
        P(),
        P("wide", "narrow"),
        P("wide", "narrow"),
        P("wide", "narrow"),
        P("narrow", "wide"),
        P(),
        P("wide", None),
        P(("groups", "wide")),
        P("groups", None),
    )
    return jax.shard_map(
        per_device,
        mesh=mesh,
        in_specs=placed,
        out_specs=(P(("groups", "wide"), None), P("groups", "narrow")),
        check_vma=False,
    )
```
